32 devices in a mesh: ga: 8 (over z, x), band: 4 (over y, core).
Axes of the slice: x: 2, y: 2, z: 4, core: 2. Of those that a mesh axis runs over, the one named last changes fastest.
Arguments:
- waves: float32 [2, 8192, 1024], P(None, 'ga', 'band'), may hold values from -6 to 6
- miller: int32 [3, 8192], P(None, 'ga'), may hold values from -8 to 8
- positions: float32 [64, 3], replicated, may hold values from 0 to 1
- form_factors: float32 [4, 18, 8192], P(None, None, 'ga'), may hold values from -0.0625 to 0.0625
- coupling: float32 [4, 18, 18], replicated, may hold values from -1.6970563 to 5.656854
- species: int32 [64], replicated, may hold values from 0 to 3
- block_sizes: int32 [64], replicated, may hold values from 1 to 18, 512 in all
- occupation: float32 [1024], P('band'), may hold values from 0.05 to 2
Outputs:
- residual: float32 [2, 8192, 1024], P(None, 'ga', 'band')
- estimate: float32 [1024], P('band')
- energy: float32 [], replicated
The draws below stay inside these ranges and needn't reach their ends.
All inputs are finite; a program needn't handle non-finite values.
Results may differ from the reference program's by a relative error of at most 0.00007.
Values sent between devices are 32-bit elements; how exact they have to be, the bound alone decides.
A program may use at most 64 MiB of HBM per device.

```python
import math
import jax
import jax.numpy as jnp
import numpy as np
from jax import lax

ATOMS = 64
KMAX = 18
NSPEC = 4
PROJ = 512
NG = 8192
NB = 1024


def draw_coupling(key, part):
    scale = (NG / (8.0 * PROJ)) ** 0.5
    first_key, second_key = jax.random.split(jax.random.fold_in(key, 11))
    offdiag = jnp.clip(0.3 * jax.random.normal(first_key, (NSPEC, KMAX, KMAX), jnp.float32), -1.2, 1.2)
    diagonal = jnp.exp(jax.random.uniform(second_key, (NSPEC, KMAX), jnp.float32, 0.0, math.log(4.0)))
    identity = jnp.eye(KMAX, dtype=jnp.float32)
    return scale * (offdiag * (1.0 - identity) + diagonal[:, :, None] * identity)


def plant(result, rng, least, top_value):
    dims = result.shape
    index_at = [jax.random.randint(jax.random.fold_in(rng, axis), (), 0, dims[axis]) for axis in range(len(dims))]
    result = result.at[tuple(index_at)].set(least)
    longest = dims.index(max(dims))
    index_at[longest] = (index_at[longest] + 1) % dims[longest]
    return result.at[tuple(index_at)].set(top_value)


def raised(result, own_key, source, target, parts, factor):
    owner, partner = [(jnp.arange(result.shape[position]) // (result.shape[position] // parts)).reshape([-1 if axis == position else 1 for axis in range(result.ndim)]) for position in (source, target)]
    chosen = jax.random.permutation(own_key, parts)[partner]
    strong = (owner == chosen) | (owner == (partner + parts // 2) % parts)
    return jnp.where(strong, factor * result, result)


def shard_levels(key, extent, cuts, low, top_value):
    def one(dim, shards_of):
        draws = jax.random.uniform(jax.random.fold_in(jax.random.fold_in(key, 6), dim), (shards_of,), jnp.float32, low / len(cuts), top_value / len(cuts))
        return jnp.repeat(jnp.exp(draws), extent[dim] // shards_of).reshape((-1,) + (1,) * (len(extent) - dim - 1))

    level = one(*cuts[0])
    for cut in cuts[1:]:
        level = level * one(*cut)
    return level


def profile(amount, total, bound, lean):
    portions = [(1 << 20) // math.isqrt(grade ** lean) + 1 for grade in range(2, amount + 1)]
    rest, holding = total - bound - (amount - 1), [1] * (amount - 1)
    while rest > 0:
        movable = [i for i in range(amount - 1) if holding[i] < bound]
        mass, left = sum([portions[i] for i in movable]), rest
        for i in movable:
            extra = min(bound - holding[i], max(1, left * portions[i] // mass), rest)
            holding[i] = holding[i] + extra
            rest = rest - extra
    return np.array([bound] + holding)


def uneven_parts(stream_key, amount, total, bound, skew):
    if amount == 2:
        one = jax.random.randint(stream_key, (), max(1, total - bound), min(bound, total - 1) + 1)
        return jnp.stack([one, total - one])
    tallies = jnp.asarray(profile(amount, total, bound, skew), jnp.int32)
    pairs = (amount - 1) // 2
    giver, receiver = tallies[1:1 + 2 * pairs:2], tallies[2:2 + 2 * pairs:2]
    slack = jnp.minimum(giver - 1, bound - receiver)
    moved = jax.random.randint(jax.random.fold_in(stream_key, 1), (pairs,), 0, 1 << 20) % (slack + 1)
    tallies = tallies.at[1:1 + 2 * pairs:2].set(giver - moved).at[2:2 + 2 * pairs:2].set(receiver + moved)
    return tallies[jax.random.permutation(jax.random.fold_in(stream_key, 2), amount)]


def scatter_about(rng, shape, spread, reach, cuts=(), kind=jnp.bfloat16):
    entries = spread * jax.random.normal(rng, shape, jnp.float32)
    if cuts:
        entries = entries * shard_levels(rng, shape, cuts, -0.22, 0.18)
    return jnp.clip(entries, -reach, reach).astype(kind)


def heavy_noise(own_key, dims, deviation, reach, cuts, heavy, kind=jnp.bfloat16):
    array = deviation * jax.random.normal(own_key, dims, jnp.float32)
    if cuts:
        array = array * shard_levels(own_key, dims, cuts, -0.22, 0.18)
    return jnp.clip(raised(array, jax.random.fold_in(own_key, 3), *heavy), -reach, reach).astype(kind)


def setup_inputs(seed: int = 0) -> dict:
    streams_of = jax.random.split(jax.random.key(seed), 9)
    waves = heavy_noise(streams_of[0], (2, NG, NB), 1.0, 6.0, ((1, 8), (2, 4)), (1, 2, 8, 2.0), jnp.float32)
    miller = plant(jax.random.randint(streams_of[1], (3, NG), -8, 9), jax.random.fold_in(streams_of[1], 1), -8, 8).astype(jnp.int32)
    positions = jnp.clip(jax.random.uniform(streams_of[2], (ATOMS, 3), jnp.float32, 0.0, 1.0), 0.0, 1.0)
    form_factors = scatter_about(streams_of[3], (NSPEC, KMAX, NG), NG ** -0.5, 0.0625, ((2, 8),), jnp.float32)
    coupling = draw_coupling(jax.random.fold_in(streams_of[8], 71), 0)
    species = plant(jax.random.randint(streams_of[5], (ATOMS,), 0, NSPEC), jax.random.fold_in(streams_of[5], 1), 0, NSPEC - 1).astype(jnp.int32)
    block_sizes = uneven_parts(streams_of[6], ATOMS, PROJ, KMAX, 1).astype(jnp.int32)
    occupation = jnp.clip(jnp.exp(math.log(2.0) - 3.6888794 * jax.random.uniform(streams_of[7], (NB,), jnp.float32) ** shard_levels(streams_of[7], (NB,), ((0, 4),), -0.2, 0.2)), 0.05, 2.0)
    return dict(waves=waves, miller=miller, positions=positions, form_factors=form_factors, coupling=coupling, species=species, block_sizes=block_sizes, occupation=occupation)


TWO_PI = 6.283185307179586
KINETIC_SCALE = 0.005
EPSILON = 1e-6
HIGHEST_PRECISION = lax.Precision.HIGHEST


def reference(waves, miller, positions, form_factors, coupling, species, block_sizes, occupation):
    block_ends = jnp.cumsum(block_sizes).astype(jnp.int32)
    block_starts = (block_ends - block_sizes).astype(jnp.int32)
    columns = jnp.arange(PROJ, dtype=jnp.int32)
    owner_atom = jnp.sum((block_ends[None, :] <= columns[:, None]).astype(jnp.int32), axis=1).astype(jnp.int32)
    channel = (columns - jnp.take(block_starts, owner_atom)).astype(jnp.int32)
    row_index = (jnp.take(species, owner_atom) * KMAX + channel).astype(jnp.int32)
    radial = jnp.take(form_factors.reshape(NSPEC * KMAX, NG), row_index, axis=0)
    miller_f = miller.astype(jnp.float32)
    phases = TWO_PI * (positions[:, 0:1] * miller_f[0][None, :] + positions[:, 1:2] * miller_f[1][None, :] + positions[:, 2:3] * miller_f[2][None, :])
    beta_re = radial * jnp.take(jnp.cos(phases), owner_atom, axis=0)
    beta_im = -(radial * jnp.take(jnp.sin(phases), owner_atom, axis=0))
    table = jnp.take(coupling.reshape(NSPEC * KMAX, KMAX), row_index, axis=0)
    dense = jnp.take(table, channel, axis=1)
    dense = jnp.where(owner_atom[:, None] == owner_atom[None, :], dense, jnp.zeros_like(dense))
    psi_re = waves[0]
    psi_im = waves[1]
    proj_re = jnp.dot(beta_re, psi_re, precision=HIGHEST_PRECISION) + jnp.dot(beta_im, psi_im, precision=HIGHEST_PRECISION)
    proj_im = jnp.dot(beta_re, psi_im, precision=HIGHEST_PRECISION) - jnp.dot(beta_im, psi_re, precision=HIGHEST_PRECISION)
    kinetic = 0.5 * KINETIC_SCALE * (miller_f[0] * miller_f[0] + miller_f[1] * miller_f[1] + miller_f[2] * miller_f[2])
    density = psi_re * psi_re + psi_im * psi_im
    kin_sum = jnp.sum(kinetic[:, None] * density, axis=0)
    norm_sum = jnp.sum(density, axis=0)
    mixed_re = jnp.dot(dense, proj_re, precision=HIGHEST_PRECISION)
    mixed_im = jnp.dot(dense, proj_im, precision=HIGHEST_PRECISION)
    nonlocal_sum = jnp.sum(proj_re * mixed_re + proj_im * mixed_im, axis=0)
    estimate = (kin_sum + nonlocal_sum) / (norm_sum + EPSILON)
    contract = (((0,), (0,)), ((), ()))
    applied_re = lax.dot_general(beta_re, mixed_re, contract, precision=HIGHEST_PRECISION) - lax.dot_general(beta_im, mixed_im, contract, precision=HIGHEST_PRECISION)
    applied_im = lax.dot_general(beta_re, mixed_im, contract, precision=HIGHEST_PRECISION) + lax.dot_general(beta_im, mixed_re, contract, precision=HIGHEST_PRECISION)
    shifted = kinetic[:, None] - estimate[None, :]
    residual = jnp.stack([shifted * psi_re + applied_re, shifted * psi_im + applied_im])
    energy = jnp.sum(occupation * nonlocal_sum / (norm_sum + EPSILON))
    return residual, estimate, energy
```

```python
import functools

import jax
import jax.numpy as jnp
from jax import lax
from jax.experimental import pallas as pl
from jax.experimental.pallas import tpu as pltpu
from jax.sharding import PartitionSpec as P

PROJ = 512
KINETIC_SCALE = 0.005
EPSILON = 1e-06
MESH = pl.DeviceIdType.MESH
F32 = jnp.float32
BF16 = jnp.bfloat16
TILE = 128
LANES = 128
COS = (1.0, -19.739208221435547, 64.93939208984375, -85.45665740966797, 60.24212646484375, -26.404630661010742, 7.800022125244141, -1.4529874324798584)
SIN = (6.2831854820251465, -41.34170150756836, 81.60513305664062, -76.7030029296875, 42.02585220336914, -14.899578094482422, 3.2377800941467285)


def split(x):
    high = x.astype(BF16)
    return high, (x - high.astype(F32)).astype(BF16)


def mm(a, b):
    return jnp.dot(a, b, preferred_element_type=F32)


def mm_t(a, b):
    return lax.dot_general(a, b, (((1,), (1,)), ((), ())), preferred_element_type=F32)


def poly(coefs, z):
    value = jnp.full_like(z, coefs[-1])
    for c in coefs[-2::-1]:
        value = value * z + c
    return value


def kernel(
    n_ga, n_band, kmax,
    waves, miller, positions, ff, coupling, species, sizes, occupation,
    residual, estimate, energy,
    beta, beta_t, psi_h, psi_l, ff_pad, cp_pad, ff_cat, cs_cat, owner_s, channel_s, crow_h, crow_l, dense_h, dense_l,
    part, landed, proj, mix_h, mix_l, stats, shares, kin_s,
    rs_send, rs_recv, ag_send, ag_recv, st_send, st_recv, en_send, en_recv,
):
    me = lax.axis_index("ga")
    my_band = lax.axis_index("band")
    rows = PROJ // n_ga
    n_blocks = PROJ // TILE
    per_block = TILE // rows
    nspec = ff.shape[0]
    kpad = -(-kmax // 8) * 8
    atoms = sizes.shape[1]
    local_g = miller.shape[1]
    bands = occupation.shape[1]

    barrier = pltpu.get_barrier_semaphore()

    def greet_ga(d, carry):
        pl.semaphore_signal(barrier, inc=1, device_id=(lax.rem(me + d, n_ga), my_band), device_id_type=MESH)
        return carry

    def greet_band(d, carry):
        pl.semaphore_signal(barrier, inc=1, device_id=(me, lax.rem(my_band + d, n_band)), device_id_type=MESH)
        return carry

    lax.fori_loop(1, n_ga, greet_ga, 0)
    lax.fori_loop(1, n_band, greet_band, 0)

    size_row = jnp.broadcast_to(sizes[...].astype(F32), (8, atoms))
    upper = (
        lax.broadcasted_iota(jnp.int32, (atoms, atoms), 0) <= lax.broadcasted_iota(jnp.int32, (atoms, atoms), 1)
    ).astype(F32).astype(BF16)
    ends = mm(size_row.astype(BF16), upper)[0:1]
    starts = ends - size_row[0:1]
    column = lax.broadcasted_iota(jnp.int32, (PROJ, atoms), 0).astype(F32)
    owner = jnp.where((column >= starts) & (column < ends), 1.0, 0.0).astype(F32)
    start_of = jnp.sum(owner * starts, axis=1, keepdims=True)
    species_of = jnp.sum(owner * species[...].astype(F32), axis=1, keepdims=True)
    channel = column[:, 0:1] - start_of
    row_index = species_of * float(kpad) + channel
    lane = lax.broadcasted_iota(jnp.int32, (PROJ, LANES), 1).astype(F32)
    row_hot = jnp.where(row_index == lane, 1.0, 0.0).astype(BF16)
    channel_s[...] = jnp.where(channel == lane, 1.0, 0.0).astype(BF16)
    blank = jnp.zeros((PROJ, LANES - atoms), BF16)
    owner_b = owner.astype(BF16)
    owner_s[:, 0:LANES] = row_hot
    owner_s[:, LANES:2 * LANES] = jnp.concatenate([owner_b, blank], axis=1)
    owner_s[:, 2 * LANES:3 * LANES] = jnp.concatenate([blank, owner_b], axis=1)

    ff_pad[...] = jnp.zeros_like(ff_pad)
    cp_pad[...] = jnp.zeros_like(cp_pad)
    for s in range(nspec):
        ff_pad[s * kpad:s * kpad + kmax, :] = ff[s]
        cp_pad[s * kpad:s * kpad + kmax, 0:kmax] = coupling[s]
    high, low = split(ff_pad[...])
    ff_cat[0:LANES] = high
    ff_cat[LANES:2 * LANES] = low

    miller_f = miller[...].astype(F32)
    turns = (
        positions[:, 0:1] * miller_f[0:1] + positions[:, 1:2] * miller_f[1:2] + positions[:, 2:3] * miller_f[2:3]
    )
    turns = turns - jnp.round(turns)
    square = turns * turns
    cosine = poly(COS, square)
    sine = turns * poly(SIN, square)
    for at, value in ((0, cosine), (LANES - atoms, sine)):
        high, low = split(value)
        cs_cat[at:at + atoms] = high
        cs_cat[LANES + at:LANES + at + atoms] = low

    for i in range(2):
        high, low = split(waves[i])
        psi_h[:, i * bands:(i + 1) * bands] = high
        psi_l[:, i * bands:(i + 1) * bands] = low

    pl.semaphore_wait(barrier, n_ga - 1 + n_band - 1)

    def rs_copy(target, source):
        return pltpu.make_async_remote_copy(
            src_ref=part.at[target], dst_ref=landed.at[source], send_sem=rs_send.at[target],
            recv_sem=rs_recv.at[source], device_id=(target, my_band), device_id_type=MESH,
        )

    my_block = me // per_block
    order = sorted(range(n_blocks), key=lambda d: -min(d, n_blocks - d))

    def project(step, carry):
        offset = order[0]
        for k in range(1, n_blocks):
            offset = jnp.where(step == k, order[k], offset)
        block = lax.rem(my_block + offset, n_blocks)
        at = pl.ds(pl.multiple_of(block * TILE, TILE), TILE)
        hot = owner_s[at, 0:LANES]
        radial = mm(jnp.concatenate([hot, hot], axis=1), ff_cat[...])
        hot = owner_s[at, LANES:2 * LANES]
        b_re = radial * mm(jnp.concatenate([hot, hot], axis=1), cs_cat[...])
        hot = owner_s[at, 2 * LANES:3 * LANES]
        b_im = -(radial * mm(jnp.concatenate([hot, hot], axis=1), cs_cat[...]))
        re_h, re_l = split(b_re)
        im_h, im_l = split(b_im)
        beta[0, at] = re_h
        beta[1, at] = im_h
        beta[2, at] = re_l
        beta[3, at] = im_l
        first = mm(jnp.concatenate([re_h, im_h, re_l, im_l], axis=0), psi_h[...])
        second = mm(jnp.concatenate([re_h, im_h], axis=0), psi_l[...])
        both = first[0:2 * TILE] + first[2 * TILE:] + second
        with_re = both[0:TILE]
        with_im = both[TILE:]
        p_re = with_re[:, 0:bands] + with_im[:, bands:]
        p_im = with_re[:, bands:] - with_im[:, 0:bands]
        for i in range(per_block):
            target = block * per_block + i
            part[target, :, 0:bands] = p_re[i * rows:(i + 1) * rows]
            part[target, :, bands:] = p_im[i * rows:(i + 1) * rows]
        for i in range(per_block):
            target = block * per_block + i

            @pl.when(target != me)
            def _():
                rs_copy(target, me).start()

        return carry

    lax.fori_loop(0, n_blocks, project, 0)

    kin_row = (
        0.5 * KINETIC_SCALE
        * (miller_f[0:1] * miller_f[0:1] + miller_f[1:2] * miller_f[1:2] + miller_f[2:3] * miller_f[2:3])
    )
    kin_s[...] = jnp.broadcast_to(kin_row, (LANES, local_g)).T
    for half in range(bands // LANES):
        lanes = pl.ds(half * LANES, LANES)
        re = waves[0, :, lanes]
        im = waves[1, :, lanes]
        density = re * re + im * im
        stats[me, 0:1, lanes] = jnp.sum(kin_s[...] * density, axis=0, keepdims=True)
        stats[me, 1:2, lanes] = jnp.sum(density, axis=0, keepdims=True)
    stats[me, 2:8] = jnp.zeros((6, bands), F32)

    def st_copy(target, source):
        return pltpu.make_async_remote_copy(
            src_ref=stats.at[source], dst_ref=stats.at[source], send_sem=st_send.at[target],
            recv_sem=st_recv.at[source], device_id=(target, my_band), device_id_type=MESH,
        )

    def each_ga(action):
        def body(d, carry):
            action(lax.rem(me + d, n_ga))
            return carry

        lax.fori_loop(1, n_ga, body, 0)

    each_ga(lambda peer: st_copy(peer, me).start())

    for k in range(4):
        def turn(block, carry):
            at = pl.ds(pl.multiple_of(block * TILE, TILE), TILE)
            to = pl.ds(pl.multiple_of((k % 2) * PROJ + block * TILE, TILE), TILE)
            beta_t[k // 2, :, to] = beta[k, at].astype(F32).T.astype(BF16)
            return carry

        lax.fori_loop(0, n_blocks, turn, 0)

    high, low = split(cp_pad[...])
    crow_h[...] = mm(owner_s[:, 0:LANES], high).astype(BF16)
    crow_l[...] = mm(owner_s[:, 0:LANES], low).astype(BF16)
    windows = [min(max(TILE * i - TILE // 2, 0), PROJ - 2 * TILE) for i in range(n_blocks)]
    for i in range(n_blocks):
        at = pl.ds(i * TILE, TILE)
        window = pl.ds(windows[i], 2 * TILE)
        same = mm_t(owner_s[at, LANES:2 * LANES], owner_s[window, LANES:2 * LANES])
        dense_h[at] = jnp.where(same > 0.5, mm_t(crow_h[at], channel_s[window]), 0.0).astype(BF16)
        dense_l[at] = jnp.where(same > 0.5, mm_t(crow_l[at], channel_s[window]), 0.0).astype(BF16)

    each_ga(lambda peer: rs_copy(me, peer).wait_recv())
    total = part[me]
    total = lax.fori_loop(1, n_ga, lambda d, t: t + landed[lax.rem(me + d, n_ga)], total)
    proj[me] = total

    def ag_copy(target, source):
        return pltpu.make_async_remote_copy(
            src_ref=proj.at[source], dst_ref=proj.at[source], send_sem=ag_send.at[target],
            recv_sem=ag_recv.at[source], device_id=(target, my_band), device_id_type=MESH,
        )

    each_ga(lambda peer: ag_copy(peer, me).start())
    each_ga(lambda peer: st_copy(me, peer).wait_recv())
    summed = stats[0]
    for s in range(1, n_ga):
        summed = summed + stats[s]
    kin_sum = summed[0:1]
    norm_sum = summed[1:2]
    each_ga(lambda peer: ag_copy(me, peer).wait_recv())

    gathered = proj[...].reshape(PROJ, 2 * bands)
    p_high, p_low = split(gathered)
    nonlocal_sum = jnp.zeros((1, bands), F32)
    for i in range(n_blocks):
        at = pl.ds(i * TILE, TILE)
        w = windows[i]
        near_h = p_high[w:w + 2 * TILE]
        near_l = p_low[w:w + 2 * TILE]
        mixed = mm(dense_h[at], near_h) + mm(dense_h[at], near_l) + mm(dense_l[at], near_h)
        product = jnp.sum(gathered[i * TILE:(i + 1) * TILE] * mixed, axis=0, keepdims=True)
        nonlocal_sum = nonlocal_sum + product[:, 0:bands] + product[:, bands:]
        below = pl.ds(PROJ + i * TILE, TILE)
        for ref, value in zip((mix_h, mix_l), split(mixed)):
            ref[at] = value
            ref[below, 0:bands] = -value[:, bands:]
            ref[below, bands:] = value[:, 0:bands]
    inverse = norm_sum + EPSILON
    quotient = (kin_sum + nonlocal_sum) / inverse
    estimate[...] = quotient
    share = jnp.sum(occupation[...] * nonlocal_sum / inverse)
    shares[my_band] = jnp.full((8, LANES), share, F32)

    def en_copy(target, source):
        return pltpu.make_async_remote_copy(
            src_ref=shares.at[source], dst_ref=shares.at[source], send_sem=en_send.at[target],
            recv_sem=en_recv.at[source], device_id=(me, target), device_id_type=MESH,
        )

    def each_band(action):
        def body(d, carry):
            action(lax.rem(my_band + d, n_band))
            return carry

        lax.fori_loop(1, n_band, body, 0)

    each_band(lambda peer: en_copy(peer, my_band).start())

    span = min(256, local_g)

    def apply(block, carry):
        at = pl.ds(pl.multiple_of(block * span, span), span)
        b_high = beta_t[0, at]
        applied = mm(b_high, mix_h[...]) + mm(beta_t[1, at], mix_h[...]) + mm(b_high, mix_l[...])
        kin = kin_s[at]
        shifted = jnp.concatenate([kin] * (bands // LANES), axis=1) - quotient
        residual[0, at] = shifted * waves[0, at] + applied[:, 0:bands]
        residual[1, at] = shifted * waves[1, at] + applied[:, bands:]
        return carry

    lax.fori_loop(0, local_g // span, apply, 0)

    each_band(lambda peer: en_copy(my_band, peer).wait_recv())
    whole = shares[0]
    for s in range(1, n_band):
        whole = whole + shares[s]
    energy[...] = whole
    each_ga(lambda peer: rs_copy(peer, me).wait_send())
    each_ga(lambda peer: st_copy(peer, me).wait_send())
    each_ga(lambda peer: ag_copy(peer, me).wait_send())
    each_band(lambda peer: en_copy(peer, my_band).wait_send())


def on_device(n_ga, n_band, waves, miller, positions, form_factors, coupling, species, block_sizes, occupation):
    nspec, kmax, local_g = form_factors.shape
    bands = waves.shape[2]
    atoms = block_sizes.shape[0]
    rows = PROJ // n_ga
    vmem = pl.BlockSpec(memory_space=pltpu.VMEM)
    dma = pltpu.SemaphoreType.DMA
    residual, estimate, energy = pl.pallas_call(
        functools.partial(kernel, n_ga, n_band, kmax),
        out_shape=(
            jax.ShapeDtypeStruct((2, local_g, bands), F32),
            jax.ShapeDtypeStruct((1, bands), F32),
            jax.ShapeDtypeStruct((8, LANES), F32),
        ),
        in_specs=[vmem] * 8,
        out_specs=(vmem, vmem, vmem),
        scratch_shapes=[
            pltpu.VMEM((4, PROJ, local_g), BF16),
            pltpu.VMEM((2, local_g, 2 * PROJ), BF16),
            pltpu.VMEM((local_g, 2 * bands), BF16),
            pltpu.VMEM((local_g, 2 * bands), BF16),
            pltpu.VMEM((LANES, local_g), F32),
            pltpu.VMEM((LANES, LANES), F32),
            pltpu.VMEM((2 * LANES, local_g), BF16),
            pltpu.VMEM((2 * LANES, local_g), BF16),
            pltpu.VMEM((PROJ, 3 * LANES), BF16),
            pltpu.VMEM((PROJ, LANES), BF16),
            pltpu.VMEM((PROJ, LANES), BF16),
            pltpu.VMEM((PROJ, LANES), BF16),
            pltpu.VMEM((PROJ, 2 * TILE), BF16),
            pltpu.VMEM((PROJ, 2 * TILE), BF16),
            pltpu.VMEM((n_ga, rows, 2 * bands), F32),
            pltpu.VMEM((n_ga, rows, 2 * bands), F32),
            pltpu.VMEM((n_ga, rows, 2 * bands), F32),
            pltpu.VMEM((2 * PROJ, 2 * bands), BF16),
            pltpu.VMEM((2 * PROJ, 2 * bands), BF16),
            pltpu.VMEM((n_ga, 8, bands), F32),
            pltpu.VMEM((n_band, 8, LANES), F32),
            pltpu.VMEM((local_g, LANES), F32),
            dma((n_ga,)), dma((n_ga,)), dma((n_ga,)), dma((n_ga,)),
            dma((n_ga,)), dma((n_ga,)), dma((n_band,)), dma((n_band,)),
        ],
        compiler_params=pltpu.CompilerParams(
            collective_id=0, has_side_effects=True, vmem_limit_bytes=48 * 1024 * 1024
        ),
    )(
        waves, miller, positions, form_factors, coupling,
        species.reshape(1, atoms), block_sizes.reshape(1, atoms), occupation.reshape(1, bands),
    )
    return residual, estimate.reshape(bands), energy[0, 0]


def solution(mesh):
    in_specs = (
        P(None, "ga", "band"),
        P(None, "ga"),
        P(),
        P(None, None, "ga"),
        P(),
        P(),
        P(),
        P("band"),
    )
    out_specs = (P(None, "ga", "band"), P("band"), P())
    body = functools.partial(on_device, mesh.shape["ga"], mesh.shape["band"])
    return jax.shard_map(body, mesh=mesh, in_specs=in_specs, out_specs=out_specs, check_vma=False)
```

```python
import functools

import jax
import jax.numpy as jnp
from jax import lax
from jax.experimental import pallas as pl
from jax.experimental.pallas import tpu as pltpu
from jax.sharding import PartitionSpec as P

PROJ = 512
KINETIC_SCALE = 0.005
EPSILON = 1e-06
MESH = pl.DeviceIdType.MESH
F32 = jnp.float32
BF16 = jnp.bfloat16
TILE = 128
LANES = 128
COS = (1.0, -19.739208221435547, 64.93939208984375, -85.45665740966797, 60.24212646484375, -26.404630661010742, 7.800022125244141, -1.4529874324798584)
SIN = (6.2831854820251465, -41.34170150756836, 81.60513305664062, -76.7030029296875, 42.02585220336914, -14.899578094482422, 3.2377800941467285)


def split(x):
    high = x.astype(BF16)
    return high, (x - high.astype(F32)).astype(BF16)


def mm(a, b):
    return jnp.dot(a, b, preferred_element_type=F32)


def mm_t(a, b):
    return lax.dot_general(a, b, (((1,), (1,)), ((), ())), preferred_element_type=F32)


def poly(coefs, z):
    value = jnp.full_like(z, coefs[-1])
    for c in coefs[-2::-1]:
        value = value * z + c
    return value


def kernel(
    n_ga, n_band, kmax,
    waves_in, miller_in, positions_in, ff_in, coupling_in, species_in, sizes_in, occupation_in,
    residual, estimate, energy,
    waves, miller, positions, ff, coupling, species, sizes, occupation,
    beta, beta_t, psi_h, psi_l, ff_pad, cp_pad, pos_pad, ff_cat, cs_cat, owner_s, channel_s, crow_h, crow_l, dense_h, dense_l,
    part, paired, landed, proj, mix_h, mix_l, stats, shares, kin_s,
    in_sems, pair_send, pair_recv, line_send, line_recv, ag_send, ag_recv, fw_send, st_send, st_recv, en_send, en_recv,
):
    me = lax.axis_index("ga")
    my_band = lax.axis_index("band")
    rows = PROJ // n_ga
    n_blocks = PROJ // TILE
    per_block = TILE // rows
    n_lines = n_ga // 2
    parity = lax.rem(me, 2)
    line = me // 2
    partner = line * 2 + 1 - parity
    nspec = ff.shape[1]
    atoms = sizes.shape[1]
    local_g = miller.shape[1]
    bands = occupation.shape[1]
    halves = bands // LANES
    wide = 2 * LANES

    loads = [
        pltpu.make_async_copy(source, target, in_sems.at[i])
        for i, (source, target) in enumerate((
            (sizes_in, sizes), (species_in, species), (positions_in, positions), (miller_in, miller),
            (ff_in, ff), (waves_in, waves), (coupling_in, coupling), (occupation_in, occupation),
        ))
    ]
    for load in loads:
        load.start()
    barrier = pltpu.get_barrier_semaphore()

    def greet_ga(d, carry):
        pl.semaphore_signal(barrier, inc=1, device_id=(lax.rem(me + d, n_ga), my_band), device_id_type=MESH)
        return carry

    def greet_band(d, carry):
        pl.semaphore_signal(barrier, inc=1, device_id=(me, lax.rem(my_band + d, n_band)), device_id_type=MESH)
        return carry

    lax.fori_loop(1, n_ga, greet_ga, 0)
    lax.fori_loop(1, n_band, greet_band, 0)

    ff_pad[...] = jnp.zeros_like(ff_pad)
    cp_pad[...] = jnp.zeros_like(cp_pad)
    pos_pad[...] = jnp.zeros_like(pos_pad)
    for load in loads[0:2]:
        load.wait()
    size_row = jnp.broadcast_to(sizes[...].astype(F32), (8, atoms))
    upper = (
        lax.broadcasted_iota(jnp.int32, (atoms, atoms), 0) <= lax.broadcasted_iota(jnp.int32, (atoms, atoms), 1)
    ).astype(F32).astype(BF16)
    ends = mm(size_row.astype(BF16), upper)[0:1]
    starts = ends - size_row[0:1]
    column = lax.broadcasted_iota(jnp.int32, (PROJ, atoms), 0).astype(F32)
    owner = jnp.where((column >= starts) & (column < ends), 1.0, 0.0).astype(F32)
    start_of = jnp.sum(owner * starts, axis=1, keepdims=True)
    species_of = jnp.sum(owner * species[...].astype(F32), axis=1, keepdims=True)
    channel = column[:, 0:1] - start_of
    row_index = channel * float(nspec) + species_of
    lane = lax.broadcasted_iota(jnp.int32, (PROJ, LANES), 1).astype(F32)
    row_hot = jnp.where(row_index == lane, 1.0, 0.0).astype(BF16)
    channel_s[...] = jnp.where(channel == lane, 1.0, 0.0).astype(BF16)
    blank = jnp.zeros((PROJ, LANES - atoms), BF16)
    owner_b = owner.astype(BF16)
    owner_s[:, 0:LANES] = row_hot
    owner_s[:, LANES:2 * LANES] = jnp.concatenate([owner_b, blank], axis=1)
    owner_s[:, 2 * LANES:3 * LANES] = jnp.concatenate([blank, owner_b], axis=1)

    for load in loads[2:4]:
        load.wait()
    pos_pad[0:3, 0:atoms] = positions[...]
    place = pos_pad[...].T[0:atoms]
    miller_f = miller[...].astype(F32)
    turns = place[:, 0:1] * miller_f[0:1] + place[:, 1:2] * miller_f[1:2] + place[:, 2:3] * miller_f[2:3]
    turns = turns - jnp.round(turns)
    square = turns * turns
    cosine = poly(COS, square)
    sine = turns * poly(SIN, square)
    for at, value in ((0, cosine), (LANES - atoms, sine)):
        high, low = split(value)
        cs_cat[at:at + atoms] = high
        cs_cat[LANES + at:LANES + at + atoms] = low

    loads[4].wait()
    for k in range(kmax):
        ff_pad[k * nspec:(k + 1) * nspec, :] = ff[k]
    high, low = split(ff_pad[...])
    ff_cat[0:LANES] = high
    ff_cat[LANES:2 * LANES] = low

    for load in loads[5:8]:
        load.wait()
    for i in range(2):
        high, low = split(waves[i])
        for h in range(halves):
            to = h * wide + i * LANES
            psi_h[:, to:to + LANES] = high[:, h * LANES:(h + 1) * LANES]
            psi_l[:, to:to + LANES] = low[:, h * LANES:(h + 1) * LANES]

    pl.semaphore_wait(barrier, n_ga - 1 + n_band - 1)

    def pair_copy(to_line):
        return pltpu.make_async_remote_copy(
            src_ref=part.at[to_line * 2 + 1 - parity], dst_ref=paired.at[to_line], send_sem=pair_send.at[to_line],
            recv_sem=pair_recv.at[to_line], device_id=(partner, my_band), device_id_type=MESH,
        )

    def line_copy(to_line, from_line):
        return pltpu.make_async_remote_copy(
            src_ref=part.at[to_line * 2 + parity], dst_ref=landed.at[from_line], send_sem=line_send.at[to_line],
            recv_sem=line_recv.at[from_line], device_id=(to_line * 2 + parity, my_band), device_id_type=MESH,
        )

    my_block = me // per_block
    lines_per_block = per_block // 2

    def block_of(step):
        rank = n_blocks - 1 - step
        swapped = 0
        bit = 1
        while bit < n_blocks:
            swapped = swapped + bit * lax.rem(lax.rem(my_block // bit, 2) + lax.rem(rank // bit, 2), 2)
            bit *= 2
        return swapped

    def pass_on(step):
        block = block_of(step)
        for i in range(lines_per_block):
            to_line = block * lines_per_block + i
            pair_copy(to_line).wait_recv()
            mine = part[to_line * 2 + parity] + paired[to_line]

            @pl.when(to_line == line)
            def _():
                landed[line] = mine

            @pl.when(to_line != line)
            def _():
                part[to_line * 2 + parity] = mine
                line_copy(to_line, line).start()

    def project(step, carry):
        block = block_of(step)
        at = pl.ds(pl.multiple_of(block * TILE, TILE), TILE)
        hot = owner_s[at, 0:LANES]
        radial = mm(jnp.concatenate([hot, hot], axis=1), ff_cat[...])
        hot = owner_s[at, LANES:2 * LANES]
        b_re = radial * mm(jnp.concatenate([hot, hot], axis=1), cs_cat[...])
        hot = owner_s[at, 2 * LANES:3 * LANES]
        b_im = -(radial * mm(jnp.concatenate([hot, hot], axis=1), cs_cat[...]))
        re_h, re_l = split(b_re)
        im_h, im_l = split(b_im)
        beta[0, at] = re_h
        beta[1, at] = im_h
        beta[2, at] = re_l
        beta[3, at] = im_l
        first = mm(jnp.concatenate([re_h, im_h, re_l, im_l], axis=0), psi_h[...])
        second = mm(jnp.concatenate([re_h, im_h], axis=0), psi_l[...])
        both = first[0:2 * TILE] + first[2 * TILE:] + second
        with_re = both[0:TILE]
        with_im = both[TILE:]
        for h in range(halves):
            a = h * wide
            b = a + LANES
            c = b + LANES
            p_re = with_re[:, a:b] + with_im[:, b:c]
            p_im = with_re[:, b:c] - with_im[:, a:b]
            for i in range(per_block):
                target = block * per_block + i
                part[target, h, :, 0:LANES] = p_re[i * rows:(i + 1) * rows]
                part[target, h, :, LANES:] = p_im[i * rows:(i + 1) * rows]
        for i in range(lines_per_block):
            pair_copy(block * lines_per_block + i).start()

        @pl.when(step > 0)
        def _():
            pass_on(step - 1)

        return carry

    lax.fori_loop(0, n_blocks, project, 0)

    kin_row = (
        0.5 * KINETIC_SCALE
        * (miller_f[0:1] * miller_f[0:1] + miller_f[1:2] * miller_f[1:2] + miller_f[2:3] * miller_f[2:3])
    )
    kin_s[...] = jnp.broadcast_to(kin_row, (LANES, local_g)).T
    for half in range(halves):
        lanes = pl.ds(half * LANES, LANES)
        re = waves[0, :, lanes]
        im = waves[1, :, lanes]
        density = re * re + im * im
        stats[me, 0:1, lanes] = jnp.sum(kin_s[...] * density, axis=0, keepdims=True)
        stats[me, 1:2, lanes] = jnp.sum(density, axis=0, keepdims=True)
    stats[me, 2:8] = jnp.zeros((6, bands), F32)

    def st_copy(target, source):
        return pltpu.make_async_remote_copy(
            src_ref=stats.at[source], dst_ref=stats.at[source], send_sem=st_send.at[target],
            recv_sem=st_recv.at[source], device_id=(target, my_band), device_id_type=MESH,
        )

    def each_ga(action):
        def body(d, carry):
            action(lax.rem(me + d, n_ga))
            return carry

        lax.fori_loop(1, n_ga, body, 0)

    each_ga(lambda peer: st_copy(peer, me).start())
    pass_on(n_blocks - 1)

    for k in range(4):
        def turn(block, carry):
            at = pl.ds(pl.multiple_of(block * TILE, TILE), TILE)
            to = pl.ds(pl.multiple_of((k % 2) * PROJ + block * TILE, TILE), TILE)
            beta_t[k // 2, :, to] = beta[k, at].astype(F32).T.astype(BF16)
            return carry

        lax.fori_loop(0, n_blocks, turn, 0)

    for k in range(kmax):
        cp_pad[k * nspec:(k + 1) * nspec, 0:kmax] = coupling[k]
    high, low = split(cp_pad[...])
    crow_h[...] = mm(owner_s[:, 0:LANES], high).astype(BF16)
    crow_l[...] = mm(owner_s[:, 0:LANES], low).astype(BF16)
    windows = [min(max(TILE * i - TILE // 2, 0), PROJ - 2 * TILE) for i in range(n_blocks)]
    for i in range(n_blocks):
        at = pl.ds(i * TILE, TILE)
        window = pl.ds(windows[i], 2 * TILE)
        same = mm_t(owner_s[at, LANES:2 * LANES], owner_s[window, LANES:2 * LANES])
        dense_h[at] = jnp.where(same > 0.5, mm_t(crow_h[at], channel_s[window]), 0.0).astype(BF16)
        dense_l[at] = jnp.where(same > 0.5, mm_t(crow_l[at], channel_s[window]), 0.0).astype(BF16)

    def each_line(action):
        def body(d, carry):
            action(lax.rem(line + d, n_lines))
            return carry

        lax.fori_loop(1, n_lines, body, 0)

    each_line(lambda other: line_copy(line, other).wait_recv())
    total = lax.fori_loop(1, n_lines, lambda d, t: t + landed[lax.rem(line + d, n_lines)], landed[line])
    for h in range(halves):
        proj[h, me] = total[h]

    def ag_copy(h, to_line, source):
        return pltpu.make_async_remote_copy(
            src_ref=proj.at[h, source], dst_ref=proj.at[h, source], send_sem=ag_send.at[h, to_line],
            recv_sem=ag_recv.at[h, source], device_id=(to_line * 2 + parity, my_band), device_id_type=MESH,
        )

    def fw_copy(h, source):
        return pltpu.make_async_remote_copy(
            src_ref=proj.at[h, source], dst_ref=proj.at[h, source], send_sem=fw_send.at[h, source // 2],
            recv_sem=ag_recv.at[h, source], device_id=(partner, my_band), device_id_type=MESH,
        )

    for h in range(halves):
        fw_copy(h, me).start()

        def send(other, h=h):
            ag_copy(h, other, me).start()

        each_line(send)

    def relay(h, d):
        source = lax.rem(line + d, n_lines) * 2 + parity
        ag_copy(h, line, source).wait_recv()
        fw_copy(h, source).start()

    def relay_first(d, carry):
        relay(0, d)
        return carry

    lax.fori_loop(1, n_lines, relay_first, 0)
    each_ga(lambda peer: st_copy(me, peer).wait_recv())
    summed = stats[0]
    for s in range(1, n_ga):
        summed = summed + stats[s]
    kin_sum = summed[0:1]
    norm_sum = summed[1:2]
    def en_copy(target, source):
        return pltpu.make_async_remote_copy(
            src_ref=shares.at[source], dst_ref=shares.at[source], send_sem=en_send.at[target],
            recv_sem=en_recv.at[source], device_id=(me, target), device_id_type=MESH,
        )

    def each_band(action):
        def body(d, carry):
            action(lax.rem(my_band + d, n_band))
            return carry

        lax.fori_loop(1, n_band, body, 0)

    inverse = norm_sum + EPSILON
    span = min(256, local_g)
    spans = local_g // span
    per_span = -(-(n_lines - 1) // spans)
    share = jnp.zeros((), F32)
    for h in range(halves):
        def arrive(d, carry, h=h):
            source = lax.rem(line + d, n_lines) * 2 + 1 - parity
            fw_copy(h, source).wait_recv()
            return carry

        lax.fori_loop(0, n_lines, arrive, 0)

        gathered = proj[h].reshape(PROJ, wide)
        p_high, p_low = split(gathered)
        nonlocal_sum = jnp.zeros((1, LANES), F32)
        for i in range(n_blocks):
            at = pl.ds(i * TILE, TILE)
            w = windows[i]
            near_h = p_high[w:w + 2 * TILE]
            near_l = p_low[w:w + 2 * TILE]
            mixed = mm(dense_h[at], near_h) + mm(dense_h[at], near_l) + mm(dense_l[at], near_h)
            product = jnp.sum(gathered[i * TILE:(i + 1) * TILE] * mixed, axis=0, keepdims=True)
            nonlocal_sum = nonlocal_sum + product[:, 0:LANES] + product[:, LANES:]
            below = pl.ds(PROJ + i * TILE, TILE)
            for ref, value in zip((mix_h, mix_l), split(mixed)):
                ref[at] = value
                ref[below, 0:LANES] = -value[:, LANES:]
                ref[below, LANES:] = value[:, 0:LANES]
        lanes = pl.ds(h * LANES, LANES)
        here = slice(h * LANES, (h + 1) * LANES)
        quotient = (kin_sum[:, here] + nonlocal_sum) / inverse[:, here]
        estimate[:, lanes] = quotient
        share = share + jnp.sum(occupation[:, lanes] * nonlocal_sum / inverse[:, here])
        if h == halves - 1:
            shares[my_band] = jnp.full((8, LANES), share, F32)
            each_band(lambda peer: en_copy(peer, my_band).start())

        def apply(block, carry, h=h, lanes=lanes, quotient=quotient):
            at = pl.ds(pl.multiple_of(block * span, span), span)
            b_high = beta_t[0, at]
            applied = mm(b_high, mix_h[...]) + mm(beta_t[1, at], mix_h[...]) + mm(b_high, mix_l[...])
            shifted = kin_s[at] - quotient
            residual[0, at, lanes] = shifted * waves[0, at, lanes] + applied[:, 0:LANES]
            residual[1, at, lanes] = shifted * waves[1, at, lanes] + applied[:, LANES:]
            if h + 1 < halves:
                for k in range(per_span):
                    d = block * per_span + k + 1

                    @pl.when(d < n_lines)
                    def _():
                        relay(h + 1, d)

            return carry

        lax.fori_loop(0, spans, apply, 0)

    each_band(lambda peer: en_copy(my_band, peer).wait_recv())
    whole = shares[0]
    for s in range(1, n_band):
        whole = whole + shares[s]
    energy[...] = whole
    def pair_done(to_line, carry):
        pair_copy(to_line).wait_send()
        return carry

    lax.fori_loop(0, n_lines, pair_done, 0)
    each_line(lambda other: line_copy(other, line).wait_send())
    for h in range(halves):
        def sent(other, h=h):
            ag_copy(h, other, me).wait_send()

        def relayed(d, carry, h=h):
            fw_copy(h, lax.rem(line + d, n_lines) * 2 + parity).wait_send()
            return carry

        each_line(sent)
        lax.fori_loop(0, n_lines, relayed, 0)
    each_ga(lambda peer: st_copy(peer, me).wait_send())
    each_band(lambda peer: en_copy(peer, my_band).wait_send())


def on_device(n_ga, n_band, waves, miller, positions, form_factors, coupling, species, block_sizes, occupation):
    nspec, kmax, local_g = form_factors.shape
    bands = waves.shape[2]
    atoms = block_sizes.shape[0]
    rows = PROJ // n_ga
    halves = bands // LANES
    vmem = pl.BlockSpec(memory_space=pltpu.VMEM)
    hbm = pl.BlockSpec(memory_space=pltpu.HBM)
    dma = pltpu.SemaphoreType.DMA
    residual, estimate, energy = pl.pallas_call(
        functools.partial(kernel, n_ga, n_band, kmax),
        out_shape=(
            jax.ShapeDtypeStruct((2, local_g, bands), F32),
            jax.ShapeDtypeStruct((1, bands), F32),
            jax.ShapeDtypeStruct((8, LANES), F32),
        ),
        in_specs=[hbm] * 8,
        out_specs=(vmem, vmem, vmem),
        scratch_shapes=[
            pltpu.VMEM((2, local_g, bands), F32),
            pltpu.VMEM((3, local_g), jnp.int32),
            pltpu.VMEM((3, atoms), F32),
            pltpu.VMEM((kmax, nspec, local_g), F32),
            pltpu.VMEM((kmax, nspec, kmax), F32),
            pltpu.VMEM((1, atoms), jnp.int32),
            pltpu.VMEM((1, atoms), jnp.int32),
            pltpu.VMEM((1, bands), F32),
            pltpu.VMEM((4, PROJ, local_g), BF16),
            pltpu.VMEM((2, local_g, 2 * PROJ), BF16),
            pltpu.VMEM((local_g, 2 * bands), BF16),
            pltpu.VMEM((local_g, 2 * bands), BF16),
            pltpu.VMEM((LANES, local_g), F32),
            pltpu.VMEM((LANES, LANES), F32),
            pltpu.VMEM((LANES, LANES), F32),
            pltpu.VMEM((2 * LANES, local_g), BF16),
            pltpu.VMEM((2 * LANES, local_g), BF16),
            pltpu.VMEM((PROJ, 3 * LANES), BF16),
            pltpu.VMEM((PROJ, LANES), BF16),
            pltpu.VMEM((PROJ, LANES), BF16),
            pltpu.VMEM((PROJ, LANES), BF16),
            pltpu.VMEM((PROJ, 2 * TILE), BF16),
            pltpu.VMEM((PROJ, 2 * TILE), BF16),
            pltpu.VMEM((n_ga, halves, rows, 2 * LANES), F32),
            pltpu.VMEM((n_ga // 2, halves, rows, 2 * LANES), F32),
            pltpu.VMEM((n_ga // 2, halves, rows, 2 * LANES), F32),
            pltpu.VMEM((halves, n_ga, rows, 2 * LANES), F32),
            pltpu.VMEM((2 * PROJ, 2 * LANES), BF16),
            pltpu.VMEM((2 * PROJ, 2 * LANES), BF16),
            pltpu.VMEM((n_ga, 8, bands), F32),
            pltpu.VMEM((n_band, 8, LANES), F32),
            pltpu.VMEM((local_g, LANES), F32),
            dma((8,)), dma((n_ga // 2,)), dma((n_ga // 2,)), dma((n_ga // 2,)), dma((n_ga // 2,)),
            dma((halves, n_ga // 2)), dma((halves, n_ga)), dma((halves, n_ga // 2)),
            dma((n_ga,)), dma((n_ga,)), dma((n_band,)), dma((n_band,)),
        ],
        compiler_params=pltpu.CompilerParams(
            collective_id=0, has_side_effects=True, vmem_limit_bytes=67_043_328
        ),
    )(
        waves, miller, positions.T, jnp.transpose(form_factors, (1, 0, 2)), jnp.transpose(coupling, (1, 0, 2)),
        species.reshape(1, atoms), block_sizes.reshape(1, atoms), occupation.reshape(1, bands),
    )
    return residual, estimate.reshape(bands), energy[0, 0]


def solution(mesh):
    in_specs = (
        P(None, "ga", "band"),
        P(None, "ga"),
        P(),
        P(None, None, "ga"),
        P(),
        P(),
        P(),
        P("band"),
    )
    out_specs = (P(None, "ga", "band"), P("band"), P())
    body = functools.partial(on_device, mesh.shape["ga"], mesh.shape["band"])
    return jax.shard_map(body, mesh=mesh, in_specs=in_specs, out_specs=out_specs, check_vma=False)
```

```python
import functools

import jax
import jax.numpy as jnp
from jax import lax
from jax.experimental import pallas as pl
from jax.experimental.pallas import tpu as pltpu
from jax.sharding import PartitionSpec as P

PROJ = 512
KINETIC_SCALE = 0.005
EPSILON = 1e-06
MESH = pl.DeviceIdType.MESH
F32 = jnp.float32
BF16 = jnp.bfloat16
TILE = 128
LANES = 128
COS = (1.0, -19.739208221435547, 64.93939208984375, -85.45665740966797, 60.24212646484375, -26.404630661010742, 7.800022125244141, -1.4529874324798584)
SIN = (6.2831854820251465, -41.34170150756836, 81.60513305664062, -76.7030029296875, 42.02585220336914, -14.899578094482422, 3.2377800941467285)


def split(x):
    high = x.astype(BF16)
    return high, (x - high.astype(F32)).astype(BF16)


def mm(a, b):
    return jnp.dot(a, b, preferred_element_type=F32)


def mm_t(a, b):
    return lax.dot_general(a, b, (((1,), (1,)), ((), ())), preferred_element_type=F32)


def poly(coefs, z):
    value = jnp.full_like(z, coefs[-1])
    for c in coefs[-2::-1]:
        value = value * z + c
    return value


def kernel(
    n_ga, n_band, kmax,
    waves_in, miller_in, positions_in, ff_in, coupling_in, species_in, sizes_in, occupation_in,
    residual, estimate, energy,
    waves, miller, positions, ff, coupling, species, sizes, occupation,
    beta, beta_t, psi_h, psi_l, ff_pad, cp_pad, pos_pad, ff_cat, cs_cat, owner_s, channel_s, crow_h, crow_l, dense_h, dense_l,
    part, paired, landed, proj, mix_h, mix_l, stats, shares, kin_s,
    in_sems, pair_send, pair_recv, line_send, line_recv, ag_send, ag_recv, fw_send, st_send, st_recv, en_send, en_recv,
):
    me = lax.axis_index("ga")
    my_band = lax.axis_index("band")
    rows = PROJ // n_ga
    n_blocks = PROJ // TILE
    per_block = TILE // rows
    n_lines = n_ga // 2
    parity = lax.rem(me, 2)
    line = me // 2
    partner = line * 2 + 1 - parity
    nspec = ff.shape[1]
    atoms = sizes.shape[1]
    local_g = miller.shape[1]
    bands = occupation.shape[1]
    halves = bands // LANES
    wide = 2 * LANES

    loads = [
        pltpu.make_async_copy(source, target, in_sems.at[i])
        for i, (source, target) in enumerate((
            (sizes_in, sizes), (species_in, species), (positions_in, positions), (miller_in, miller),
            (ff_in, ff), (waves_in, waves), (coupling_in, coupling), (occupation_in, occupation),
        ))
    ]
    for load in loads:
        load.start()
    barrier = pltpu.get_barrier_semaphore()

    def greet_ga(d, carry):
        pl.semaphore_signal(barrier, inc=1, device_id=(lax.rem(me + d, n_ga), my_band), device_id_type=MESH)
        return carry

    def greet_band(d, carry):
        pl.semaphore_signal(barrier, inc=1, device_id=(me, lax.rem(my_band + d, n_band)), device_id_type=MESH)
        return carry

    lax.fori_loop(1, n_ga, greet_ga, 0)
    lax.fori_loop(1, n_band, greet_band, 0)

    ff_pad[...] = jnp.zeros_like(ff_pad)
    cp_pad[...] = jnp.zeros_like(cp_pad)
    pos_pad[...] = jnp.zeros_like(pos_pad)
    for load in loads[0:2]:
        load.wait()
    size_row = jnp.broadcast_to(sizes[...].astype(F32), (8, atoms))
    upper = (
        lax.broadcasted_iota(jnp.int32, (atoms, atoms), 0) <= lax.broadcasted_iota(jnp.int32, (atoms, atoms), 1)
    ).astype(F32).astype(BF16)
    ends = mm(size_row.astype(BF16), upper)[0:1]
    starts = ends - size_row[0:1]
    column = lax.broadcasted_iota(jnp.int32, (PROJ, atoms), 0).astype(F32)
    owner = jnp.where((column >= starts) & (column < ends), 1.0, 0.0).astype(F32)
    start_of = jnp.sum(owner * starts, axis=1, keepdims=True)
    species_of = jnp.sum(owner * species[...].astype(F32), axis=1, keepdims=True)
    channel = column[:, 0:1] - start_of
    row_index = channel * float(nspec) + species_of
    lane = lax.broadcasted_iota(jnp.int32, (PROJ, LANES), 1).astype(F32)
    row_hot = jnp.where(row_index == lane, 1.0, 0.0).astype(BF16)
    channel_s[...] = jnp.where(channel == lane, 1.0, 0.0).astype(BF16)
    blank = jnp.zeros((PROJ, LANES - atoms), BF16)
    owner_b = owner.astype(BF16)
    owner_s[:, 0:LANES] = row_hot
    owner_s[:, LANES:2 * LANES] = jnp.concatenate([owner_b, blank], axis=1)
    owner_s[:, 2 * LANES:3 * LANES] = jnp.concatenate([blank, owner_b], axis=1)

    for load in loads[2:4]:
        load.wait()
    pos_pad[0:3, 0:atoms] = positions[...]
    place = pos_pad[...].T[0:atoms]
    miller_f = miller[...].astype(F32)
    turns = place[:, 0:1] * miller_f[0:1] + place[:, 1:2] * miller_f[1:2] + place[:, 2:3] * miller_f[2:3]
    turns = turns - jnp.round(turns)
    square = turns * turns
    cosine = poly(COS, square)
    sine = turns * poly(SIN, square)
    for at, value in ((0, cosine), (LANES - atoms, sine)):
        high, low = split(value)
        cs_cat[at:at + atoms] = high
        cs_cat[LANES + at:LANES + at + atoms] = low

    loads[4].wait()
    for k in range(kmax):
        ff_pad[k * nspec:(k + 1) * nspec, :] = ff[k]
    high, low = split(ff_pad[...])
    ff_cat[0:LANES] = high
    ff_cat[LANES:2 * LANES] = low

    for load in loads[5:8]:
        load.wait()
    for i in range(2):
        high, low = split(waves[i])
        for h in range(halves):
            to = h * wide + i * LANES
            psi_h[:, to:to + LANES] = high[:, h * LANES:(h + 1) * LANES]
            psi_l[:, to:to + LANES] = low[:, h * LANES:(h + 1) * LANES]

    pl.semaphore_wait(barrier, n_ga - 1 + n_band - 1)

    def pair_copy(to_line):
        return pltpu.make_async_remote_copy(
            src_ref=part.at[to_line * 2 + 1 - parity], dst_ref=paired.at[to_line], send_sem=pair_send.at[to_line],
            recv_sem=pair_recv.at[to_line], device_id=(partner, my_band), device_id_type=MESH,
        )

    def line_copy(to_line, from_line):
        return pltpu.make_async_remote_copy(
            src_ref=part.at[to_line * 2 + parity], dst_ref=landed.at[from_line], send_sem=line_send.at[to_line],
            recv_sem=line_recv.at[from_line], device_id=(to_line * 2 + parity, my_band), device_id_type=MESH,
        )

    my_block = me // per_block
    lines_per_block = per_block // 2

    def block_of(step):
        rank = n_blocks - 1 - step
        swapped = 0
        bit = 1
        while bit < n_blocks:
            swapped = swapped + bit * lax.rem(lax.rem(my_block // bit, 2) + lax.rem(rank // bit, 2), 2)
            bit *= 2
        return swapped

    def pass_on(step):
        block = block_of(step)
        for i in range(lines_per_block):
            to_line = block * lines_per_block + i
            pair_copy(to_line).wait_recv()
            mine = part[to_line * 2 + parity] + paired[to_line]

            @pl.when(to_line == line)
            def _():
                landed[line] = mine

            @pl.when(to_line != line)
            def _():
                part[to_line * 2 + parity] = mine
                line_copy(to_line, line).start()

    def project(step, carry):
        block = block_of(step)
        at = pl.ds(pl.multiple_of(block * TILE, TILE), TILE)
        hot = owner_s[at, 0:LANES]
        radial = mm(jnp.concatenate([hot, hot], axis=1), ff_cat[...])
        hot = owner_s[at, LANES:2 * LANES]
        b_re = radial * mm(jnp.concatenate([hot, hot], axis=1), cs_cat[...])
        hot = owner_s[at, 2 * LANES:3 * LANES]
        b_im = -(radial * mm(jnp.concatenate([hot, hot], axis=1), cs_cat[...]))
        re_h, re_l = split(b_re)
        im_h, im_l = split(b_im)
        beta[0, at] = re_h
        beta[1, at] = im_h
        beta[2, at] = re_l
        beta[3, at] = im_l
        first = mm(jnp.concatenate([re_h, im_h, re_l, im_l], axis=0), psi_h[...])
        second = mm(jnp.concatenate([re_h, im_h], axis=0), psi_l[...])
        both = first[0:2 * TILE] + first[2 * TILE:] + second
        with_re = both[0:TILE]
        with_im = both[TILE:]
        for h in range(halves):
            a = h * wide
            b = a + LANES
            c = b + LANES
            p_re = with_re[:, a:b] + with_im[:, b:c]
            p_im = with_re[:, b:c] - with_im[:, a:b]
            for i in range(per_block):
                target = block * per_block + i
                part[target, h, :, 0:LANES] = p_re[i * rows:(i + 1) * rows]
                part[target, h, :, LANES:] = p_im[i * rows:(i + 1) * rows]
        for i in range(lines_per_block):
            pair_copy(block * lines_per_block + i).start()

        @pl.when(step > 0)
        def _():
            pass_on(step - 1)

        return carry

    lax.fori_loop(0, n_blocks, project, 0)

    kin_row = (
        0.5 * KINETIC_SCALE
        * (miller_f[0:1] * miller_f[0:1] + miller_f[1:2] * miller_f[1:2] + miller_f[2:3] * miller_f[2:3])
    )
    kin_s[...] = jnp.broadcast_to(kin_row, (LANES, local_g)).T
    for half in range(halves):
        lanes = pl.ds(half * LANES, LANES)
        re = waves[0, :, lanes]
        im = waves[1, :, lanes]
        density = re * re + im * im
        stats[me, 0:1, lanes] = jnp.sum(kin_s[...] * density, axis=0, keepdims=True)
        stats[me, 1:2, lanes] = jnp.sum(density, axis=0, keepdims=True)
    stats[me, 2:8] = jnp.zeros((6, bands), F32)

    def st_copy(target, source):
        return pltpu.make_async_remote_copy(
            src_ref=stats.at[source], dst_ref=stats.at[source], send_sem=st_send.at[target],
            recv_sem=st_recv.at[source], device_id=(target, my_band), device_id_type=MESH,
        )

    def each_ga(action):
        def body(d, carry):
            action(lax.rem(me + d, n_ga))
            return carry

        lax.fori_loop(1, n_ga, body, 0)

    each_ga(lambda peer: st_copy(peer, me).start())
    pass_on(n_blocks - 1)

    for k in range(4):
        def turn(block, carry):
            at = pl.ds(pl.multiple_of(block * TILE, TILE), TILE)
            to = pl.ds(pl.multiple_of((k % 2) * PROJ + block * TILE, TILE), TILE)
            beta_t[k // 2, :, to] = beta[k, at].astype(F32).T.astype(BF16)
            return carry

        lax.fori_loop(0, n_blocks, turn, 0)

    for k in range(kmax):
        cp_pad[k * nspec:(k + 1) * nspec, 0:kmax] = coupling[k]
    high, low = split(cp_pad[...])
    crow_h[...] = mm(owner_s[:, 0:LANES], high).astype(BF16)
    crow_l[...] = mm(owner_s[:, 0:LANES], low).astype(BF16)
    windows = [min(max(TILE * i - TILE // 2, 0), PROJ - 2 * TILE) for i in range(n_blocks)]
    for i in range(n_blocks):
        at = pl.ds(i * TILE, TILE)
        window = pl.ds(windows[i], 2 * TILE)
        same = mm_t(owner_s[at, LANES:2 * LANES], owner_s[window, LANES:2 * LANES])
        dense_h[at] = jnp.where(same > 0.5, mm_t(crow_h[at], channel_s[window]), 0.0).astype(BF16)
        dense_l[at] = jnp.where(same > 0.5, mm_t(crow_l[at], channel_s[window]), 0.0).astype(BF16)

    def each_line(action):
        def body(d, carry):
            action(lax.rem(line + d, n_lines))
            return carry

        lax.fori_loop(1, n_lines, body, 0)

    each_line(lambda other: line_copy(line, other).wait_recv())
    total = lax.fori_loop(1, n_lines, lambda d, t: t + landed[lax.rem(line + d, n_lines)], landed[line])
    for h in range(halves):
        proj[h, me] = total[h]

    def ag_copy(h, to_line, source):
        return pltpu.make_async_remote_copy(
            src_ref=proj.at[h, source], dst_ref=proj.at[h, source], send_sem=ag_send.at[h, to_line],
            recv_sem=ag_recv.at[h, source], device_id=(to_line * 2 + parity, my_band), device_id_type=MESH,
        )

    def fw_copy(h, source):
        return pltpu.make_async_remote_copy(
            src_ref=proj.at[h, source], dst_ref=proj.at[h, source], send_sem=fw_send.at[h, source // 2],
            recv_sem=ag_recv.at[h, source], device_id=(partner, my_band), device_id_type=MESH,
        )

    for h in range(halves):
        fw_copy(h, me).start()

        def send(other, h=h):
            ag_copy(h, other, me).start()

        each_line(send)

    def relay(h, d):
        source = lax.rem(line + n_lines - d, n_lines) * 2 + parity
        ag_copy(h, line, source).wait_recv()
        fw_copy(h, source).start()

    def relay_first(d, carry):
        relay(0, d)
        return carry

    lax.fori_loop(1, n_lines, relay_first, 0)
    each_ga(lambda peer: st_copy(me, peer).wait_recv())
    summed = stats[0]
    for s in range(1, n_ga):
        summed = summed + stats[s]
    kin_sum = summed[0:1]
    norm_sum = summed[1:2]
    def en_copy(target, source):
        return pltpu.make_async_remote_copy(
            src_ref=shares.at[source], dst_ref=shares.at[source], send_sem=en_send.at[target],
            recv_sem=en_recv.at[source], device_id=(me, target), device_id_type=MESH,
        )

    def each_band(action):
        def body(d, carry):
            action(lax.rem(my_band + d, n_band))
            return carry

        lax.fori_loop(1, n_band, body, 0)

    inverse = norm_sum + EPSILON
    span = min(256, local_g)
    spans = local_g // span
    per_span = -(-(n_lines - 1) // spans)
    share = jnp.zeros((), F32)
    for h in range(halves):
        def arrive(d, carry, h=h):
            source = lax.rem(line + d, n_lines) * 2 + 1 - parity
            fw_copy(h, source).wait_recv()
            return carry

        lax.fori_loop(0, n_lines, arrive, 0)

        gathered = proj[h].reshape(PROJ, wide)
        p_high, p_low = split(gathered)
        nonlocal_sum = jnp.zeros((1, LANES), F32)
        for i in range(n_blocks):
            at = pl.ds(i * TILE, TILE)
            w = windows[i]
            near_h = p_high[w:w + 2 * TILE]
            near_l = p_low[w:w + 2 * TILE]
            mixed = mm(dense_h[at], near_h) + mm(dense_h[at], near_l) + mm(dense_l[at], near_h)
            product = jnp.sum(gathered[i * TILE:(i + 1) * TILE] * mixed, axis=0, keepdims=True)
            nonlocal_sum = nonlocal_sum + product[:, 0:LANES] + product[:, LANES:]
            below = pl.ds(PROJ + i * TILE, TILE)
            for ref, value in zip((mix_h, mix_l), split(mixed)):
                ref[at] = value
                ref[below, 0:LANES] = -value[:, LANES:]
                ref[below, LANES:] = value[:, 0:LANES]
        lanes = pl.ds(h * LANES, LANES)
        here = slice(h * LANES, (h + 1) * LANES)
        quotient = (kin_sum[:, here] + nonlocal_sum) / inverse[:, here]
        estimate[:, lanes] = quotient
        share = share + jnp.sum(occupation[:, lanes] * nonlocal_sum / inverse[:, here])
        if h == halves - 1:
            shares[my_band] = jnp.full((8, LANES), share, F32)
            each_band(lambda peer: en_copy(peer, my_band).start())

        def apply(block, carry, h=h, lanes=lanes, quotient=quotient):
            at = pl.ds(pl.multiple_of(block * span, span), span)
            b_high = beta_t[0, at]
            applied = mm(b_high, mix_h[...]) + mm(beta_t[1, at], mix_h[...]) + mm(b_high, mix_l[...])
            shifted = kin_s[at] - quotient
            residual[0, at, lanes] = shifted * waves[0, at, lanes] + applied[:, 0:LANES]
            residual[1, at, lanes] = shifted * waves[1, at, lanes] + applied[:, LANES:]
            if h + 1 < halves:
                for k in range(per_span):
                    d = block * per_span + k + 1

                    @pl.when(d < n_lines)
                    def _():
                        relay(h + 1, d)

            return carry

        lax.fori_loop(0, spans, apply, 0)

    each_band(lambda peer: en_copy(my_band, peer).wait_recv())
    whole = shares[0]
    for s in range(1, n_band):
        whole = whole + shares[s]
    energy[...] = whole[0:1, 0:1]
    def pair_done(to_line, carry):
        pair_copy(to_line).wait_send()
        return carry

    lax.fori_loop(0, n_lines, pair_done, 0)
    each_line(lambda other: line_copy(other, line).wait_send())
    for h in range(halves):
        def sent(other, h=h):
            ag_copy(h, other, me).wait_send()

        def relayed(d, carry, h=h):
            fw_copy(h, lax.rem(line + d, n_lines) * 2 + parity).wait_send()
            return carry

        each_line(sent)
        lax.fori_loop(0, n_lines, relayed, 0)
    each_ga(lambda peer: st_copy(peer, me).wait_send())
    each_band(lambda peer: en_copy(peer, my_band).wait_send())


def on_device(n_ga, n_band, waves, miller, positions, form_factors, coupling, species, block_sizes, occupation):
    nspec, kmax, local_g = form_factors.shape
    bands = waves.shape[2]
    atoms = block_sizes.shape[0]
    rows = PROJ // n_ga
    halves = bands // LANES
    vmem = pl.BlockSpec(memory_space=pltpu.VMEM)
    hbm = pl.BlockSpec(memory_space=pltpu.HBM)
    dma = pltpu.SemaphoreType.DMA
    residual, estimate, energy = pl.pallas_call(
        functools.partial(kernel, n_ga, n_band, kmax),
        out_shape=(
            jax.ShapeDtypeStruct((2, local_g, bands), F32),
            jax.ShapeDtypeStruct((1, bands), F32),
            jax.ShapeDtypeStruct((1, 1), F32),
        ),
        in_specs=[hbm] * 8,
        out_specs=(vmem, vmem, vmem),
        scratch_shapes=[
            pltpu.VMEM((2, local_g, bands), F32),
            pltpu.VMEM((3, local_g), jnp.int32),
            pltpu.VMEM((3, atoms), F32),
            pltpu.VMEM((kmax, nspec, local_g), F32),
            pltpu.VMEM((kmax, nspec, kmax), F32),
            pltpu.VMEM((1, atoms), jnp.int32),
            pltpu.VMEM((1, atoms), jnp.int32),
            pltpu.VMEM((1, bands), F32),
            pltpu.VMEM((4, PROJ, local_g), BF16),
            pltpu.VMEM((2, local_g, 2 * PROJ), BF16),
            pltpu.VMEM((local_g, 2 * bands), BF16),
            pltpu.VMEM((local_g, 2 * bands), BF16),
            pltpu.VMEM((LANES, local_g), F32),
            pltpu.VMEM((LANES, LANES), F32),
            pltpu.VMEM((LANES, LANES), F32),
            pltpu.VMEM((2 * LANES, local_g), BF16),
            pltpu.VMEM((2 * LANES, local_g), BF16),
            pltpu.VMEM((PROJ, 3 * LANES), BF16),
            pltpu.VMEM((PROJ, LANES), BF16),
            pltpu.VMEM((PROJ, LANES), BF16),
            pltpu.VMEM((PROJ, LANES), BF16),
            pltpu.VMEM((PROJ, 2 * TILE), BF16),
            pltpu.VMEM((PROJ, 2 * TILE), BF16),
            pltpu.VMEM((n_ga, halves, rows, 2 * LANES), F32),
            pltpu.VMEM((n_ga // 2, halves, rows, 2 * LANES), F32),
            pltpu.VMEM((n_ga // 2, halves, rows, 2 * LANES), F32),
            pltpu.VMEM((halves, n_ga, rows, 2 * LANES), F32),
            pltpu.VMEM((2 * PROJ, 2 * LANES), BF16),
            pltpu.VMEM((2 * PROJ, 2 * LANES), BF16),
            pltpu.VMEM((n_ga, 8, bands), F32),
            pltpu.VMEM((n_band, 8, LANES), F32),
            pltpu.VMEM((local_g, LANES), F32),
            dma((8,)), dma((n_ga // 2,)), dma((n_ga // 2,)), dma((n_ga // 2,)), dma((n_ga // 2,)),
            dma((halves, n_ga // 2)), dma((halves, n_ga)), dma((halves, n_ga // 2)),
            dma((n_ga,)), dma((n_ga,)), dma((n_band,)), dma((n_band,)),
        ],
        compiler_params=pltpu.CompilerParams(
            collective_id=0, has_side_effects=True, vmem_limit_bytes=67_043_328
        ),
    )(
        waves, miller, positions.T, jnp.transpose(form_factors, (1, 0, 2)), jnp.transpose(coupling, (1, 0, 2)),
        species.reshape(1, atoms), block_sizes.reshape(1, atoms), occupation.reshape(1, bands),
    )
    return residual, estimate.reshape(bands), energy.reshape(())


def solution(mesh):
    in_specs = (
        P(None, "ga", "band"),
        P(None, "ga"),
        P(),
        P(None, None, "ga"),
        P(),
        P(),
        P(),
        P("band"),
    )
    out_specs = (P(None, "ga", "band"), P("band"), P())
    body = functools.partial(on_device, mesh.shape["ga"], mesh.shape["band"])
    return jax.shard_map(body, mesh=mesh, in_specs=in_specs, out_specs=out_specs, check_vma=False)
```
